32 devices in a mesh: gx: 4 (over z), gy: 4 (over x, core), gz: 2 (over y).
Axes of the slice: x: 2, y: 2, z: 4, core: 2. Of those that a mesh axis runs over, the one named last changes fastest.
Arguments:
- coords: float32 [3, 4, 1024, 128], P(None, 'gx', ('gy', 'gz')), may hold values from 0 to 11
- charges: float32 [4, 1024, 128], P('gx', ('gy', 'gz')), may hold values from -1.5 to 1.5
- atom_types: int32 [4, 1024, 128], P('gx', ('gy', 'gz')), may hold values from 0 to 63
- lj_sigma: float32 [64], replicated, may hold values from 2 to 4
- lj_epsilon: float32 [64], replicated, may hold values from 0.02 to 0.25
- tile_list: int32 [4, 4, 2, 2, 512], P('gx', 'gy', 'gz'), may hold values from -1 to 3455, as said below
Outputs:
- forces: float32 [3, 4, 1024, 128], P(None, 'gx', ('gy', 'gz'))
The draws below stay inside these ranges and needn't reach their ends.
Inputs may be any that keep to these rules, and one draw needn't show every extreme that they name: tile_list[x, y, z, 0, t] is a block of brick (x, y, z) (0 to 127) and tile_list[x, y, z, 1, t] a block of its neighbourhood whose cell touches the home block's cell or is that cell (cell indices differ by at most one along each dimension, counted across brick faces periodically); on each brick the listed tiles come first and the remaining slots hold -1 in both rows; at least 256 tiles are listed on every brick and all 512 on some brick; tiles may repeat.
All inputs are finite; a program needn't handle non-finite values.
Results may differ from the reference program's by a relative error of at most 0.0003.
Values sent between devices are 32-bit elements; how exact they have to be, the bound alone decides.
A program may use at most 128 MiB of HBM per device.

```python
import math
import jax
import jax.numpy as jnp
from jax import lax

GRID = 4
LAYERS = 8
BLOCKS = 128
TILES = 512
TYPES = 64
ATOMS_BLOCK = 128
SLAB = 1024
N_GX = 4
N_GY = 4
N_GZ = 2


def draw_tile_list(key, part):
    devices = N_GX * N_GY * N_GZ
    key_home, key_step, key_count, key_full = jax.random.split(jax.random.fold_in(key, 7), 4)
    home_ids = jax.random.randint(key_home, (devices, TILES), 0, BLOCKS)
    step = jax.random.randint(key_step, (devices, TILES), 0, 27)
    cell_x = home_ids // (GRID * LAYERS) + step // 9 - 1
    cell_y = home_ids // LAYERS % GRID + step // 3 % 3 - 1
    cell_z = home_ids % LAYERS + step % 3 - 1
    off_x = (cell_x >= GRID).astype(jnp.int32) - (cell_x < 0).astype(jnp.int32)
    off_y = (cell_y >= GRID).astype(jnp.int32) - (cell_y < 0).astype(jnp.int32)
    off_z = (cell_z >= LAYERS).astype(jnp.int32) - (cell_z < 0).astype(jnp.int32)
    cell_x = cell_x - off_x * GRID
    cell_y = cell_y - off_y * GRID
    cell_z = cell_z - off_z * LAYERS
    slot = 9 * (off_x + 1) + 3 * (off_y + 1) + (off_z + 1)
    source_ids = slot * BLOCKS + (cell_x * GRID + cell_y) * LAYERS + cell_z
    listed = jax.random.randint(key_count, (devices,), TILES // 2, TILES + 1)
    fullest = jax.random.randint(key_full, (), 0, devices)
    listed = jnp.where(jnp.arange(devices) == fullest, TILES, listed)
    alive = jnp.arange(TILES)[None, :] < listed[:, None]
    home_ids = jnp.where(alive, home_ids, -1)
    source_ids = jnp.where(alive, source_ids, -1)
    return jnp.stack([home_ids, source_ids], 1).reshape(N_GX, N_GY, N_GZ, 2, TILES).astype(jnp.int32)


def touch_ends(values, own_key, least, largest):
    index_at = [jax.random.randint(jax.random.fold_in(own_key, axis), (), 0, length) for axis, length in enumerate(values.shape)]
    main_axis = values.shape.index(max(values.shape))
    next_to = index_at[:main_axis] + [(index_at[main_axis] + 1) % values.shape[main_axis]] + index_at[main_axis + 1:]
    return values.at[tuple(index_at)].set(least).at[tuple(next_to)].set(largest)


def block_levels(own_key, extent, cuts, least, largest):
    def one(position, parts):
        draws = jax.random.uniform(jax.random.fold_in(jax.random.fold_in(own_key, 6), position), (parts,), jnp.float32, least / len(cuts), largest / len(cuts))
        return jnp.repeat(jnp.exp(draws), extent[position] // parts).reshape((-1,) + (1,) * (len(extent) - position - 1))

    gain = one(*cuts[0])
    for cut in cuts[1:]:
        gain = gain * one(*cut)
    return gain


def normal_values(own_key, extent, spread, bound, shards=(), kind=jnp.bfloat16):
    array = spread * jax.random.normal(own_key, extent, jnp.float32)
    if shards:
        array = array * block_levels(own_key, extent, shards, -0.22, 0.18)
    return jnp.clip(array, -bound, bound).astype(kind)


def setup_inputs(seed: int = 0) -> dict:
    splits = jax.random.split(jax.random.key(seed), 7)
    return {
        "coords": jnp.clip(11.0 * jax.random.uniform(splits[0], (3, N_GX, SLAB, ATOMS_BLOCK), jnp.float32) ** block_levels(splits[0], (3, N_GX, SLAB, ATOMS_BLOCK), ((1, 4), (2, 8)), -0.2, 0.2), 0.0, 11.0),
        "charges": normal_values(splits[1], (N_GX, SLAB, ATOMS_BLOCK), 0.3, 1.5, ((0, 4), (1, 8)), jnp.float32),
        "atom_types": touch_ends(jax.random.randint(splits[2], (N_GX, SLAB, ATOMS_BLOCK), 0, TYPES), jax.random.fold_in(splits[2], 1), 0, TYPES - 1).astype(jnp.int32),
        "lj_sigma": jnp.clip(jax.random.uniform(splits[3], (TYPES,), jnp.float32, 2.0, 4.0), 2.0, 4.0),
        "lj_epsilon": jnp.clip(jnp.exp(jax.random.uniform(splits[4], (TYPES,), jnp.float32, math.log(0.02), math.log(0.25))), 0.02, 0.25),
        "tile_list": draw_tile_list(jax.random.fold_in(splits[6], 71), 0),
    }


cell_edge = 11.0
cutoff = 9.0
soft_core = 16.0
coulomb = 332.0636

def radial(softened, sigma_pair, eps_pair, charge_pair):
    ratio = sigma_pair * sigma_pair / softened
    cubed = ratio * ratio * ratio
    return 24.0 * eps_pair * (2.0 * cubed * cubed - cubed) / softened + charge_pair / (softened * jnp.sqrt(softened))

def tile_forces(home_block, source_block):
    delta = home_block[:3, :, :, None] - source_block[:3, :, None, :]
    dist_sq = lax.optimization_barrier(jnp.sum(delta * delta, axis=0))
    softened = dist_sq + soft_core
    sigma_pair = 0.5 * (home_block[4][:, :, None] + source_block[4][:, None, :])
    eps_pair = home_block[5][:, :, None] * source_block[5][:, None, :]
    charge_pair = coulomb * home_block[3][:, :, None] * source_block[3][:, None, :]
    limit = jnp.full_like(softened, cutoff * cutoff + soft_core)
    shifted = radial(softened, sigma_pair, eps_pair, charge_pair) - radial(limit, sigma_pair, eps_pair, charge_pair)
    strength = jnp.where(dist_sq < cutoff * cutoff, shifted, jnp.zeros_like(shifted))
    return lax.optimization_barrier(jnp.sum(strength[None] * delta, axis=3))

def brick_forces(home_atoms, region, tile_ids):
    count = tile_ids.shape[1]
    group = min(64, count)
    grouped = tile_ids.reshape(2, count // group, group).transpose(1, 0, 2)
    blocks = home_atoms.shape[1]
    rows = jnp.arange(blocks, dtype=jnp.int32)

    def advance(totals, pair_ids):
        home_block = jnp.take(home_atoms, jnp.maximum(pair_ids[0], 0), axis=1)
        source_block = jnp.take(region, jnp.maximum(pair_ids[1], 0), axis=1)
        pushes = tile_forces(home_block, source_block)
        selector = (pair_ids[0][None, :] == rows[:, None]).astype(totals.dtype)
        added = jnp.einsum('bg,cga->cba', selector, pushes, precision=lax.Precision.HIGHEST)
        return (totals + added, None)
    start = jnp.zeros((3,) + home_atoms.shape[1:], home_atoms.dtype)
    return lax.scan(advance, start, grouped)[0]

def cell_corners(dtype, grid, layers):
    block = jnp.arange(grid * grid * layers, dtype=jnp.int32)
    return jnp.stack([block // (grid * layers), block // layers % grid, block % layers]).astype(dtype) * cell_edge

def slot_offsets(dtype, grid, layers):
    slot = jnp.arange(27, dtype=jnp.int32)
    steps = jnp.stack([(slot // 9 - 1) * grid, (slot // 3 % 3 - 1) * grid, (slot % 3 - 1) * layers])
    return steps.astype(dtype) * cell_edge

def reference(coords, charges, atom_types, lj_sigma, lj_epsilon, tile_list):
    atoms = jnp.concatenate([coords, charges[None], lj_sigma[atom_types][None], jnp.sqrt(lj_epsilon)[atom_types][None]], 0)
    per_brick = atoms.reshape(6, N_GX, BLOCKS, N_GY, N_GZ, ATOMS_BLOCK).transpose(1, 3, 4, 0, 2, 5)
    corners = cell_corners(coords.dtype, GRID, LAYERS)
    per_brick = jnp.concatenate([per_brick[:, :, :, :3] + corners[:, :, None], per_brick[:, :, :, 3:]], 3)
    offsets = slot_offsets(coords.dtype, GRID, LAYERS)
    slots = jnp.arange(27, dtype=jnp.int32)

    def one_brick(brick):
        xpos = brick // (N_GY * N_GZ)
        ypos = brick // N_GZ % N_GY
        zpos = brick % N_GZ
        nearby = per_brick[(xpos + slots // 9 - 1) % N_GX, (ypos + slots // 3 % 3 - 1) % N_GY, (zpos + slots % 3 - 1) % N_GZ]
        region = jnp.concatenate([nearby[:, :3] + offsets.T[:, :, None, None], nearby[:, 3:]], 1)
        region = region.transpose(1, 0, 2, 3).reshape(6, 27 * BLOCKS, ATOMS_BLOCK)
        return brick_forces(per_brick[xpos, ypos, zpos], region, tile_list[xpos, ypos, zpos])
    result = lax.map(one_brick, jnp.arange(N_GX * N_GY * N_GZ, dtype=jnp.int32))
    result = result.reshape(N_GX, N_GY, N_GZ, 3, BLOCKS, ATOMS_BLOCK).transpose(3, 0, 4, 1, 2, 5)
    return result.reshape(3, N_GX, BLOCKS * N_GY * N_GZ, ATOMS_BLOCK)
```

```python
import functools

import jax
import jax.numpy as jnp
from jax import lax
from jax.experimental import pallas as pl
from jax.experimental.pallas import tpu as pltpu
from jax.sharding import PartitionSpec as P

GRID = 4
ROWS = 8

cell_edge = 11.0
cutoff = 9.0
soft_core = 16.0
coulomb = 332.0636
limit = cutoff * cutoff + soft_core
sigma_scale = 0.5 * 2.0 ** (1.0 / 6.0)
root_scale = 12.0**0.5
charge_scale = coulomb**0.5


def extended(block, sides, width):
    for axis, dim in sides:
        count = lax.axis_size(axis)
        forward = [(i, i + 1) for i in range(count - 1)]
        forward.append((count - 1, 0))
        backward = [(target, source) for source, target in forward]
        low = lax.ppermute(
            lax.slice_in_dim(block, block.shape[dim] - width, None, axis=dim), axis, forward
        )
        high = lax.ppermute(lax.slice_in_dim(block, 0, width, axis=dim), axis, backward)
        block = jnp.concatenate([low, block, high], axis=dim)
    return block


def powers(softened):
    root = lax.rsqrt(softened)
    one = root * root
    two = one * one
    four = two * two
    return one * root, four, four * (two * one)


def force_kernel(pairs, count, region, out, totals):
    width = region.shape[2]
    half, four_at, seven_at = powers(jnp.full((8, width), limit, jnp.float32))

    totals[...] = jnp.zeros_like(totals)

    def tile(index):
        home = pairs[1, index]
        source = region[pairs[2, index]].T
        mine = [jnp.broadcast_to(region[home, k : k + 1, :], (8, width)) for k in range(6)]
        sums = None
        for group in range(width // 8):
            part = source[group * 8 : group * 8 + 8, :]
            x, y, z, charge, sigma, root = [
                jnp.broadcast_to(part[:, k : k + 1], (8, width)) for k in range(6)
            ]
            dx, dy, dz = mine[0] - x, mine[1] - y, mine[2] - z
            softened = jnp.minimum(dx * dx + dy * dy + (dz * dz + soft_core), limit)
            near, four, seven = powers(softened)
            width_pair = mine[4] + sigma
            square = width_pair * width_pair
            sixth = square * square * square
            strength = (mine[5] * root * sixth) * (
                sixth * (seven - seven_at) - (four - four_at)
            ) + (mine[3] * charge) * (near - half)
            pushed = (strength * dx, strength * dy, strength * dz)
            sums = pushed if sums is None else tuple(a + b for a, b in zip(sums, pushed))
        row = pairs[0, index]
        for axis in range(3):
            totals[axis, pl.ds(row, 1), :] += jnp.sum(sums[axis], axis=0, keepdims=True)

    def step(index, carry):
        tile(2 * index)
        tile(2 * index + 1)
        return carry

    lax.fori_loop(0, (count[0] + 1) // 2, step, 0)
    out[...] = totals[:, : out.shape[1], :]


def brick_forces(region, pairs, count, blocks):
    width = region.shape[2]
    return pl.pallas_call(
        force_kernel,
        out_shape=jax.ShapeDtypeStruct((3, blocks, width), jnp.float32),
        in_specs=[
            pl.BlockSpec(memory_space=pltpu.SMEM),
            pl.BlockSpec(memory_space=pltpu.SMEM),
            pl.BlockSpec(memory_space=pltpu.VMEM),
        ],
        out_specs=pl.BlockSpec(memory_space=pltpu.VMEM),
        scratch_shapes=[pltpu.VMEM((3, blocks + 8, width), jnp.float32)],
    )(pairs, count, region)


def rim_shift(length, inner, dtype):
    index = jnp.arange(length + 2, dtype=jnp.int32)
    return ((index == length + 1).astype(jnp.int32) - (index == 0).astype(jnp.int32)).astype(
        dtype
    ) * (inner * cell_edge)


def per_device(coords, charges, atom_types, lj_sigma, lj_epsilon, tile_list):
    span_y = lax.axis_size("gy")
    span_z = lax.axis_size("gz")
    blocks = coords.shape[2]
    width = coords.shape[3]
    layers = blocks // (GRID * GRID)
    ranks = span_y * span_z
    stride = blocks // ranks
    dtype = coords.dtype
    kinds = jnp.arange(lj_sigma.shape[0], dtype=jnp.int32)
    selector = (atom_types[0][:, :, None] == kinds).astype(dtype)
    sigma_atom = jnp.sum(selector * (lj_sigma * sigma_scale), axis=2)
    root_atom = jnp.sum(selector * (jnp.sqrt(lj_epsilon) * root_scale), axis=2)
    rank = lax.axis_index("gy") * span_z + lax.axis_index("gz")
    cell = rank * stride + jnp.arange(blocks, dtype=jnp.int32) // ranks
    corner = [
        (place.astype(dtype) * cell_edge)[:, None]
        for place in (cell // (GRID * layers), cell // layers % GRID, cell % layers)
    ]
    zero = jnp.zeros_like(sigma_atom)
    atoms = jnp.stack(
        [coords[k, 0] + corner[k] for k in range(3)]
        + [charges[0] * charge_scale, sigma_atom, root_atom, zero, zero],
        axis=1,
    )
    outgoing = atoms.reshape(stride, ranks, ROWS, width)
    arrived = lax.all_to_all(outgoing, ("gy", "gz"), split_axis=1, concat_axis=0, tiled=True)
    cells = arrived.reshape(GRID, GRID, layers, ROWS, width)
    padded = extended(cells, (("gx", 0), ("gy", 1), ("gz", 2)), 1)
    shape_pad = (GRID + 2, GRID + 2, layers + 2)
    lines = (
        rim_shift(GRID, GRID, dtype)[:, None, None],
        rim_shift(GRID, GRID, dtype)[None, :, None],
        rim_shift(layers, layers, dtype)[None, None, :],
    )
    axis_row = jnp.arange(ROWS, dtype=jnp.int32)
    shifts = sum(
        jnp.where(axis_row == k, jnp.broadcast_to(line, shape_pad)[..., None], 0.0)
        for k, line in enumerate(lines)
    )
    region = (padded + shifts[..., None]).reshape(-1, ROWS, width)
    pairs = tile_list[0, 0, 0]
    dead = pairs[0] < 0

    def place(ids):
        ids = jnp.maximum(ids, 0)
        slot = ids // blocks
        member = ids % blocks
        px = member // (GRID * layers) + (slot // 9 - 1) * GRID + 1
        py = member // layers % GRID + (slot // 3 % 3 - 1) * GRID + 1
        pz = member % layers + (slot % 3 - 1) * layers + 1
        return jnp.where(dead, 0, (px * (GRID + 2) + py) * (layers + 2) + pz)

    table = jnp.stack(
        [jnp.where(dead, blocks, pairs[0]), place(pairs[0] + 13 * blocks), place(pairs[1])]
    )
    count = jnp.sum((~dead).astype(jnp.int32)).reshape(1)
    totals = brick_forces(region, table, count, blocks)
    sending = totals.reshape(3, ranks, stride, width)[:, :, :, None]
    returned = lax.all_to_all(sending, ("gy", "gz"), split_axis=1, concat_axis=3, tiled=True)
    return returned.reshape(3, 1, blocks, width)


def solution(mesh):
    return jax.shard_map(
        per_device,
        mesh=mesh,
        in_specs=(
            P(None, "gx", ("gy", "gz"), None),
            P("gx", ("gy", "gz"), None),
            P("gx", ("gy", "gz"), None),
            P(),
            P(),
            P("gx", "gy", "gz", None, None),
        ),
        out_specs=P(None, "gx", ("gy", "gz"), None),
        check_vma=False,
    )
```

```python
import functools

import jax
import jax.numpy as jnp
from jax import lax
from jax.experimental import pallas as pl
from jax.experimental.pallas import tpu as pltpu
from jax.sharding import PartitionSpec as P

GRID = 4
ROWS = 8
BATCH = 4

cell_edge = 11.0
cutoff = 9.0
soft_core = 16.0
coulomb = 332.0636
limit = cutoff * cutoff + soft_core
sigma_scale = 0.5 * 2.0 ** (1.0 / 6.0)
root_scale = 12.0**0.5
charge_scale = coulomb**0.5


def extended(block, sides, width):
    for axis, dim in sides:
        count = lax.axis_size(axis)
        forward = [(i, i + 1) for i in range(count - 1)]
        forward.append((count - 1, 0))
        backward = [(target, source) for source, target in forward]
        low = lax.ppermute(
            lax.slice_in_dim(block, block.shape[dim] - width, None, axis=dim), axis, forward
        )
        high = lax.ppermute(lax.slice_in_dim(block, 0, width, axis=dim), axis, backward)
        block = jnp.concatenate([low, block, high], axis=dim)
    return block


def powers(softened):
    root = lax.rsqrt(softened)
    one = root * root
    two = one * one
    four = two * two
    return one * root, four, four * (two * one)


def split(value):
    high = value.astype(jnp.bfloat16).astype(jnp.float32)
    rest = value - high
    middle = rest.astype(jnp.bfloat16).astype(jnp.float32)
    return high, middle, rest - middle


def stacked(parts):
    return jnp.concatenate(parts, axis=0).astype(jnp.bfloat16)


def source_stack(source):
    high, middle, low = split(source)
    return stacked([high, middle, high, middle, high, low])


def home_stack(home):
    high, middle, low = split(home)
    return stacked([high, high, middle, middle, low, high])


def moved_home(pairs, index, region):
    home = region[pairs[1, index]]
    lane_row = lax.broadcasted_iota(jnp.int32, home.shape, 0)
    step = [pairs[3 + k, index].astype(jnp.float32) * cell_edge for k in range(3)]
    offset = jnp.where(
        lane_row == 0, step[0], jnp.where(lane_row == 1, step[1], jnp.where(lane_row == 2, step[2], 0.0))
    )
    return home, home - offset, lane_row


def pair_terms(pairs, index, region, terms):
    home, moved, lane_row = moved_home(pairs, index, region)
    square = jnp.sum(jnp.where(lane_row < 3, moved * moved, 0.0), axis=0, keepdims=True)
    ones = jnp.where(lane_row == 4, 1.0, 0.0)
    distance = jnp.where(lane_row < 3, -2.0 * moved, jnp.where(lane_row == 3, square, ones))
    sigma = jnp.where(lane_row == 3, home[5:6, :], jnp.where(lane_row == 5, 1.0, 0.0))
    root = jnp.where(lane_row == 6, home, 0.0)
    charge = jnp.where(lane_row == 7, home, 0.0)
    wide = jnp.concatenate([distance, sigma, root, charge], axis=1)
    terms[...] = lax.dot_general(
        source_stack(region[pairs[2, index]]),
        home_stack(wide),
        (((0,), (0,)), ((), ())),
        preferred_element_type=jnp.float32,
    )


def strengths(terms, high, low, at_limit):
    width = terms.shape[0]
    near_at, four_at, seven_at = at_limit
    for start in range(0, width, 16):
        rows = pl.ds(start, 16)
        softened, sigma, root, charge = [
            terms[rows, k * width : (k + 1) * width] for k in range(4)
        ]
        near, four, seven = powers(jnp.minimum(softened, limit))
        square = sigma * sigma
        sixth = square * square * square
        strength = (root * sixth) * (
            sixth * (seven - seven_at) - (four - four_at)
        ) + charge * (near - near_at)
        top = strength.astype(jnp.bfloat16)
        high[rows, :] = top
        low[rows, :] = (strength - top.astype(jnp.float32)).astype(jnp.bfloat16)


def add_forces(pairs, index, region, high, low, totals):
    _, moved, _ = moved_home(pairs, index, region)
    top, middle, _ = split(region[pairs[2, index]])
    weights = stacked([top, middle])
    both = jnp.dot(weights, high[...], preferred_element_type=jnp.float32) + jnp.dot(
        weights, low[...], preferred_element_type=jnp.float32
    )
    summed = both[:ROWS] + both[ROWS:]
    totals[pairs[0, index]] += moved * summed[3:4, :] - summed


def force_kernel(pairs, count, region, out, totals, *slots):
    width = region.shape[2]
    at_limit = powers(jnp.full((16, width), limit, jnp.float32))
    totals[...] = jnp.zeros_like(totals)
    terms = (slots[:BATCH], slots[BATCH : 2 * BATCH])
    highs = (slots[2 * BATCH : 3 * BATCH], slots[3 * BATCH : 4 * BATCH])
    lows = (slots[4 * BATCH : 5 * BATCH], slots[5 * BATCH :])

    def step(index, carry):
        for turn in range(2):
            first = (2 * index + turn) * BATCH
            for t in range(BATCH):
                add_forces(pairs, first + t, region, highs[turn][t], lows[turn][t], totals)
                strengths(terms[1 - turn][t], highs[1 - turn][t], lows[1 - turn][t], at_limit)
                pair_terms(pairs, first + 2 * BATCH + t, region, terms[turn][t])
        return carry

    groups = (count[0] + BATCH - 1) // BATCH
    lax.fori_loop(0, (groups + 3) // 2, step, 0)
    for axis in range(3):
        out[axis] = totals[: out.shape[1], axis, :]


def brick_forces(region, pairs, count, blocks):
    width = region.shape[2]
    return pl.pallas_call(
        force_kernel,
        out_shape=jax.ShapeDtypeStruct((3, blocks, width), jnp.float32),
        in_specs=[
            pl.BlockSpec(memory_space=pltpu.SMEM),
            pl.BlockSpec(memory_space=pltpu.SMEM),
            pl.BlockSpec(memory_space=pltpu.VMEM),
        ],
        out_specs=pl.BlockSpec(memory_space=pltpu.VMEM),
        scratch_shapes=[pltpu.VMEM((blocks + 1, ROWS, width), jnp.float32)]
        + [pltpu.VMEM((width, 4 * width), jnp.float32)] * (2 * BATCH)
        + [pltpu.VMEM((width, width), jnp.bfloat16)] * (4 * BATCH),
    )(pairs, count, region)


def per_device(coords, charges, atom_types, lj_sigma, lj_epsilon, tile_list):
    span_y = lax.axis_size("gy")
    span_z = lax.axis_size("gz")
    blocks = coords.shape[2]
    width = coords.shape[3]
    layers = blocks // (GRID * GRID)
    ranks = span_y * span_z
    stride = blocks // ranks
    dtype = coords.dtype
    kinds = jnp.arange(lj_sigma.shape[0], dtype=jnp.int32)
    selector = (atom_types[0][:, :, None] == kinds).astype(dtype)
    sigma_atom = jnp.sum(selector * (lj_sigma * sigma_scale), axis=2)
    root_atom = jnp.sum(selector * (jnp.sqrt(lj_epsilon) * root_scale), axis=2)
    inner = coords[:, 0] - 0.5 * cell_edge
    square = inner[0] * inner[0] + inner[1] * inner[1] + inner[2] * inner[2] + soft_core
    atoms = jnp.stack(
        [inner[0], inner[1], inner[2], jnp.ones_like(square), square]
        + [sigma_atom, root_atom, charges[0] * charge_scale],
        axis=1,
    )
    outgoing = atoms.reshape(stride, ranks, ROWS, width)
    arrived = lax.all_to_all(outgoing, ("gy", "gz"), split_axis=1, concat_axis=0, tiled=True)
    cells = arrived.reshape(GRID, GRID, layers, ROWS, width)
    padded = extended(cells, (("gx", 0), ("gy", 1), ("gz", 2)), 1)
    region = padded.reshape(-1, ROWS, width)
    pairs = jnp.pad(
        tile_list[0, 0, 0], ((0, 0), (2 * BATCH, 4 * BATCH)), constant_values=-1
    )
    dead = pairs[0] < 0

    def place(ids):
        slot = ids // blocks
        member = ids % blocks
        px = member // (GRID * layers) + (slot // 9 - 1) * GRID
        py = member // layers % GRID + (slot // 3 % 3 - 1) * GRID
        pz = member % layers + (slot % 3 - 1) * layers
        return px, py, pz

    own = place(jnp.where(dead, 0, pairs[0]) + 13 * blocks)
    other = place(jnp.where(dead, 13 * blocks, pairs[1]))
    lines = [
        ((x + 1) * (GRID + 2) + y + 1) * (layers + 2) + z + 1 for x, y, z in (own, other)
    ]
    table = jnp.stack(
        [jnp.where(dead, blocks, pairs[0])] + lines + [b - a for a, b in zip(own, other)]
    )
    count = jnp.sum((~dead).astype(jnp.int32)).reshape(1)
    totals = brick_forces(region, table, count, blocks)
    sending = totals.reshape(3, ranks, stride, width)[:, :, :, None]
    returned = lax.all_to_all(sending, ("gy", "gz"), split_axis=1, concat_axis=3, tiled=True)
    return returned.reshape(3, 1, blocks, width)


def solution(mesh):
    return jax.shard_map(
        per_device,
        mesh=mesh,
        in_specs=(
            P(None, "gx", ("gy", "gz"), None),
            P("gx", ("gy", "gz"), None),
            P("gx", ("gy", "gz"), None),
            P(),
            P(),
            P("gx", "gy", "gz", None, None),
        ),
        out_specs=P(None, "gx", ("gy", "gz"), None),
        check_vma=False,
    )
```

```python
import itertools
import math

import jax
import jax.numpy as jnp
from jax import lax
from jax.experimental import pallas as pl
from jax.experimental.pallas import tpu as pltpu
from jax.sharding import PartitionSpec as P

GRID = 4
ROWS = 8
BATCH = 4

cell_edge = 11.0
cutoff = 9.0
soft_core = 16.0
coulomb = 332.0636
limit = cutoff * cutoff + soft_core
sigma_scale = 0.5 * 2.0 ** (1.0 / 6.0)
root_scale = 12.0**0.5
charge_scale = coulomb**0.5


def exchange_kernel(atoms, region, send_own, recv_own, send_rim, recv_rim, own_sem):
    stride, ranks = atoms.shape[:2]
    layers = region.shape[2] - 2
    spans = [lax.axis_size(name) for name in ("gx", "gy", "gz")]
    here = [lax.axis_index(name) for name in ("gx", "gy", "gz")]
    me = here[1] * spans[2] + here[2]
    chunk = math.gcd(stride, layers)
    pieces = stride // chunk

    def place(piece):
        cell = me * stride + piece * chunk
        return region.at[
            cell // (GRID * layers) + 1,
            lax.rem(cell // layers, GRID) + 1,
            pl.ds(lax.rem(cell, layers) + 1, chunk),
        ]

    copies = []
    for hop in range(1, ranks):
        to = lax.rem(me + hop, ranks)
        for piece in range(pieces):
            sem = (hop - 1) * pieces + piece
            copies.append(
                pltpu.make_async_remote_copy(
                    src_ref=atoms.at[pl.ds(piece * chunk, chunk), to],
                    dst_ref=place(piece),
                    send_sem=send_own.at[sem],
                    recv_sem=recv_own.at[sem],
                    device_id=(here[0], to // spans[2], lax.rem(to, spans[2])),
                    device_id_type=pl.DeviceIdType.MESH,
                )
            )
            copies[-1].start()
    for piece in range(pieces):
        kept = pltpu.make_async_copy(
            atoms.at[pl.ds(piece * chunk, chunk), me], place(piece), own_sem.at[piece]
        )
        kept.start()
        copies.append(kept)
    for copy in copies:
        copy.wait()

    lengths = (GRID, GRID, layers)
    rims = []
    offsets = [o for o in itertools.product((-1, 0, 1), repeat=3) if any(o)]
    for sem, offset in enumerate(offsets):
        source = tuple(
            pl.ds(1, n) if o == 0 else pl.ds(n if o > 0 else 1, 1)
            for o, n in zip(offset, lengths)
        )
        target = tuple(
            pl.ds(1, n) if o == 0 else pl.ds(0 if o > 0 else n + 1, 1)
            for o, n in zip(offset, lengths)
        )
        rims.append(
            pltpu.make_async_remote_copy(
                src_ref=region.at[source],
                dst_ref=region.at[target],
                send_sem=send_rim.at[sem],
                recv_sem=recv_rim.at[sem],
                device_id=tuple(
                    lax.rem(at + o + n, n) for at, o, n in zip(here, offset, spans)
                ),
                device_id_type=pl.DeviceIdType.MESH,
            )
        )
        rims[-1].start()
    for copy in rims:
        copy.wait()


def exchanged(atoms, layers):
    stride, ranks, rows, width = atoms.shape
    pieces = stride // math.gcd(stride, layers)
    own = pltpu.SemaphoreType.DMA(((ranks - 1) * pieces,))
    rim = pltpu.SemaphoreType.DMA((26,))
    return pl.pallas_call(
        exchange_kernel,
        out_shape=jax.ShapeDtypeStruct(
            (GRID + 2, GRID + 2, layers + 2, rows, width), atoms.dtype
        ),
        in_specs=[pl.BlockSpec(memory_space=pltpu.VMEM)],
        out_specs=pl.BlockSpec(memory_space=pltpu.VMEM),
        scratch_shapes=[own, own, rim, rim, pltpu.SemaphoreType.DMA((pieces,))],
        compiler_params=pltpu.CompilerParams(has_side_effects=True),
    )(atoms)


def powers(softened):
    root = lax.rsqrt(softened)
    one = root * root
    two = one * one
    four = two * two
    return one * root, four, four * (two * one)


def split(value):
    high = value.astype(jnp.bfloat16).astype(jnp.float32)
    rest = value - high
    middle = rest.astype(jnp.bfloat16).astype(jnp.float32)
    return high, middle, rest - middle


def stacked(parts):
    return jnp.concatenate(parts, axis=0).astype(jnp.bfloat16)


def source_stack(source):
    high, middle, low = split(source)
    return stacked([high, middle, high, middle, high, low])


def home_stack(home):
    high, middle, low = split(home)
    return stacked([high, high, middle, middle, low, high])


def moved_home(pairs, index, region):
    home = region[pairs[1, index]]
    lane_row = lax.broadcasted_iota(jnp.int32, home.shape, 0)
    step = [pairs[3 + k, index].astype(jnp.float32) * cell_edge for k in range(3)]
    offset = jnp.where(
        lane_row == 0, step[0], jnp.where(lane_row == 1, step[1], jnp.where(lane_row == 2, step[2], 0.0))
    )
    return home, home - offset, lane_row


def pair_terms(pairs, index, region, terms):
    home, moved, lane_row = moved_home(pairs, index, region)
    square = jnp.sum(jnp.where(lane_row < 3, moved * moved, 0.0), axis=0, keepdims=True)
    ones = jnp.where(lane_row == 4, 1.0, 0.0)
    distance = jnp.where(lane_row < 3, -2.0 * moved, jnp.where(lane_row == 3, square, ones))
    sigma = jnp.where(lane_row == 3, home[5:6, :], jnp.where(lane_row == 5, 1.0, 0.0))
    root = jnp.where(lane_row == 6, home, 0.0)
    charge = jnp.where(lane_row == 7, home, 0.0)
    wide = jnp.concatenate([distance, sigma, root, charge], axis=1)
    terms[...] = lax.dot_general(
        source_stack(region[pairs[2, index]]),
        home_stack(wide),
        (((0,), (0,)), ((), ())),
        preferred_element_type=jnp.float32,
    )


def strengths(terms, high, low, at_limit):
    width = terms.shape[0]
    near_at, four_at, seven_at = at_limit
    for start in range(0, width, 16):
        rows = pl.ds(start, 16)
        softened, sigma, root, charge = [
            terms[rows, k * width : (k + 1) * width] for k in range(4)
        ]
        near, four, seven = powers(jnp.minimum(softened, limit))
        square = sigma * sigma
        sixth = square * square * square
        strength = (root * sixth) * (
            sixth * (seven - seven_at) - (four - four_at)
        ) + charge * (near - near_at)
        top = strength.astype(jnp.bfloat16)
        high[rows, :] = top
        low[rows, :] = (strength - top.astype(jnp.float32)).astype(jnp.bfloat16)


def add_forces(pairs, index, region, high, low, totals):
    _, moved, _ = moved_home(pairs, index, region)
    top, middle, _ = split(region[pairs[2, index]])
    weights = stacked([top, middle])
    both = jnp.dot(weights, high[...], preferred_element_type=jnp.float32) + jnp.dot(
        weights, low[...], preferred_element_type=jnp.float32
    )
    summed = both[:ROWS] + both[ROWS:]
    totals[pairs[0, index]] += moved * summed[3:4, :] - summed


def force_kernel(pairs, count, region, out, totals, *slots):
    width = region.shape[2]
    at_limit = powers(jnp.full((16, width), limit, jnp.float32))
    totals[...] = jnp.zeros_like(totals)
    terms = (slots[:BATCH], slots[BATCH : 2 * BATCH])
    highs = (slots[2 * BATCH : 3 * BATCH], slots[3 * BATCH : 4 * BATCH])
    lows = (slots[4 * BATCH : 5 * BATCH], slots[5 * BATCH :])

    def step(index, carry):
        for turn in range(2):
            first = (2 * index + turn) * BATCH
            for t in range(BATCH):
                add_forces(pairs, first + t, region, highs[turn][t], lows[turn][t], totals)
                strengths(terms[1 - turn][t], highs[1 - turn][t], lows[1 - turn][t], at_limit)
                pair_terms(pairs, first + 2 * BATCH + t, region, terms[turn][t])
        return carry

    groups = (count[0] + BATCH - 1) // BATCH
    lax.fori_loop(0, (groups + 3) // 2, step, 0)
    for axis in range(3):
        out[axis] = totals[: out.shape[1], axis, :]


def brick_forces(region, pairs, count, blocks):
    width = region.shape[2]
    return pl.pallas_call(
        force_kernel,
        out_shape=jax.ShapeDtypeStruct((3, blocks, width), jnp.float32),
        in_specs=[
            pl.BlockSpec(memory_space=pltpu.SMEM),
            pl.BlockSpec(memory_space=pltpu.SMEM),
            pl.BlockSpec(memory_space=pltpu.VMEM),
        ],
        out_specs=pl.BlockSpec(memory_space=pltpu.VMEM),
        scratch_shapes=[pltpu.VMEM((blocks + 1, ROWS, width), jnp.float32)]
        + [pltpu.VMEM((width, 4 * width), jnp.float32)] * (2 * BATCH)
        + [pltpu.VMEM((width, width), jnp.bfloat16)] * (4 * BATCH),
    )(pairs, count, region)


def per_device(coords, charges, atom_types, lj_sigma, lj_epsilon, tile_list):
    span_y = lax.axis_size("gy")
    span_z = lax.axis_size("gz")
    blocks = coords.shape[2]
    width = coords.shape[3]
    layers = blocks // (GRID * GRID)
    ranks = span_y * span_z
    stride = blocks // ranks
    dtype = coords.dtype
    kinds = jnp.arange(lj_sigma.shape[0], dtype=jnp.int32)
    selector = (atom_types[0][:, :, None] == kinds).astype(dtype)
    sigma_atom = jnp.sum(selector * (lj_sigma * sigma_scale), axis=2)
    root_atom = jnp.sum(selector * (jnp.sqrt(lj_epsilon) * root_scale), axis=2)
    inner = coords[:, 0] - 0.5 * cell_edge
    square = inner[0] * inner[0] + inner[1] * inner[1] + inner[2] * inner[2] + soft_core
    atoms = jnp.stack(
        [inner[0], inner[1], inner[2], jnp.ones_like(square), square]
        + [sigma_atom, root_atom, charges[0] * charge_scale],
        axis=1,
    )
    outgoing = atoms.reshape(stride, ranks, ROWS, width)
    padded = exchanged(outgoing, layers)
    region = padded.reshape(-1, ROWS, width)
    pairs = jnp.pad(
        tile_list[0, 0, 0], ((0, 0), (2 * BATCH, 4 * BATCH)), constant_values=-1
    )
    dead = pairs[0] < 0

    def place(ids):
        slot = ids // blocks
        member = ids % blocks
        px = member // (GRID * layers) + (slot // 9 - 1) * GRID
        py = member // layers % GRID + (slot // 3 % 3 - 1) * GRID
        pz = member % layers + (slot % 3 - 1) * layers
        return px, py, pz

    own = place(jnp.where(dead, 0, pairs[0]) + 13 * blocks)
    other = place(jnp.where(dead, 13 * blocks, pairs[1]))
    lines = [
        ((x + 1) * (GRID + 2) + y + 1) * (layers + 2) + z + 1 for x, y, z in (own, other)
    ]
    table = jnp.stack(
        [jnp.where(dead, blocks, pairs[0])] + lines + [b - a for a, b in zip(own, other)]
    )
    count = jnp.sum((~dead).astype(jnp.int32)).reshape(1)
    totals = brick_forces(region, table, count, blocks)
    sending = totals.reshape(3, ranks, stride, width)[:, :, :, None]
    returned = lax.all_to_all(sending, ("gy", "gz"), split_axis=1, concat_axis=3, tiled=True)
    return returned.reshape(3, 1, blocks, width)


def solution(mesh):
    return jax.shard_map(
        per_device,
        mesh=mesh,
        in_specs=(
            P(None, "gx", ("gy", "gz"), None),
            P("gx", ("gy", "gz"), None),
            P("gx", ("gy", "gz"), None),
            P(),
            P(),
            P("gx", "gy", "gz", None, None),
        ),
        out_specs=P(None, "gx", ("gy", "gz"), None),
        check_vma=False,
    )
```

```python
import itertools
import math

import jax
import jax.numpy as jnp
from jax import lax
from jax.experimental import pallas as pl
from jax.experimental.pallas import tpu as pltpu
from jax.sharding import PartitionSpec as P

GRID = 4
ROWS = 8
BATCH = 8

cell_edge = 11.0
cutoff = 9.0
soft_core = 16.0
coulomb = 332.0636
limit = cutoff * cutoff + soft_core
sigma_scale = 0.5 * 2.0 ** (1.0 / 6.0)
root_scale = 12.0**0.5
charge_scale = coulomb**0.5


def exchange_kernel(atoms, region, send_own, recv_own, send_rim, recv_rim, own_sem):
    stride, ranks = atoms.shape[:2]
    layers = region.shape[2] - 2
    spans = [lax.axis_size(name) for name in ("gx", "gy", "gz")]
    here = [lax.axis_index(name) for name in ("gx", "gy", "gz")]
    me = here[1] * spans[2] + here[2]
    chunk = math.gcd(stride, layers)
    pieces = stride // chunk

    def place(piece):
        cell = me * stride + piece * chunk
        return region.at[
            cell // (GRID * layers) + 1,
            lax.rem(cell // layers, GRID) + 1,
            pl.ds(lax.rem(cell, layers) + 1, chunk),
        ]

    copies = []
    for hop in range(1, ranks):
        to = lax.rem(me + hop, ranks)
        for piece in range(pieces):
            sem = (hop - 1) * pieces + piece
            copies.append(
                pltpu.make_async_remote_copy(
                    src_ref=atoms.at[pl.ds(piece * chunk, chunk), to],
                    dst_ref=place(piece),
                    send_sem=send_own.at[sem],
                    recv_sem=recv_own.at[sem],
                    device_id=(here[0], to // spans[2], lax.rem(to, spans[2])),
                    device_id_type=pl.DeviceIdType.MESH,
                )
            )
            copies[-1].start()
    for piece in range(pieces):
        kept = pltpu.make_async_copy(
            atoms.at[pl.ds(piece * chunk, chunk), me], place(piece), own_sem.at[piece]
        )
        kept.start()
        copies.append(kept)
    for copy in copies:
        copy.wait()

    lengths = (GRID, GRID, layers)
    rims = []
    offsets = [o for o in itertools.product((-1, 0, 1), repeat=3) if any(o)]
    for sem, offset in enumerate(offsets):
        source = tuple(
            pl.ds(1, n) if o == 0 else pl.ds(n if o > 0 else 1, 1)
            for o, n in zip(offset, lengths)
        )
        target = tuple(
            pl.ds(1, n) if o == 0 else pl.ds(0 if o > 0 else n + 1, 1)
            for o, n in zip(offset, lengths)
        )
        rims.append(
            pltpu.make_async_remote_copy(
                src_ref=region.at[source],
                dst_ref=region.at[target],
                send_sem=send_rim.at[sem],
                recv_sem=recv_rim.at[sem],
                device_id=tuple(
                    lax.rem(at + o + n, n) for at, o, n in zip(here, offset, spans)
                ),
                device_id_type=pl.DeviceIdType.MESH,
            )
        )
        rims[-1].start()
    for copy in rims:
        copy.wait()


def exchanged(atoms, layers):
    stride, ranks, rows, width = atoms.shape
    pieces = stride // math.gcd(stride, layers)
    own = pltpu.SemaphoreType.DMA(((ranks - 1) * pieces,))
    rim = pltpu.SemaphoreType.DMA((26,))
    return pl.pallas_call(
        exchange_kernel,
        out_shape=jax.ShapeDtypeStruct(
            (GRID + 2, GRID + 2, layers + 2, rows, width), atoms.dtype
        ),
        in_specs=[pl.BlockSpec(memory_space=pltpu.VMEM)],
        out_specs=pl.BlockSpec(memory_space=pltpu.VMEM),
        scratch_shapes=[own, own, rim, rim, pltpu.SemaphoreType.DMA((pieces,))],
        compiler_params=pltpu.CompilerParams(has_side_effects=True),
    )(atoms)


def powers(softened):
    root = lax.rsqrt(softened)
    one = root * root
    two = one * one
    four = two * two
    return one * root, four, four * (two * one)


def split(value):
    high = value.astype(jnp.bfloat16).astype(jnp.float32)
    rest = value - high
    middle = rest.astype(jnp.bfloat16).astype(jnp.float32)
    return high, middle, rest - middle


def stacked(parts):
    return jnp.concatenate(parts, axis=0).astype(jnp.bfloat16)


def source_stack(source):
    high, middle, low = split(source)
    return stacked([high, middle, high, middle, high, low])


def home_stack(home):
    high, middle, low = split(home)
    return stacked([high, high, middle, middle, low, high])


def moved_home(pairs, index, region):
    home = region[pairs[1, index]]
    lane_row = lax.broadcasted_iota(jnp.int32, home.shape, 0)
    step = [pairs[3 + k, index].astype(jnp.float32) * cell_edge for k in range(3)]
    offset = jnp.where(
        lane_row == 0, step[0], jnp.where(lane_row == 1, step[1], jnp.where(lane_row == 2, step[2], 0.0))
    )
    return home, home - offset, lane_row


def pair_terms(pairs, index, region, terms):
    home, moved, lane_row = moved_home(pairs, index, region)
    square = jnp.sum(jnp.where(lane_row < 3, moved * moved, 0.0), axis=0, keepdims=True)
    ones = jnp.where(lane_row == 4, 1.0, 0.0)
    distance = jnp.where(lane_row < 3, -2.0 * moved, jnp.where(lane_row == 3, square, ones))
    sigma = jnp.where(lane_row == 3, home[5:6, :], jnp.where(lane_row == 5, 1.0, 0.0))
    root = jnp.where(lane_row == 6, home, 0.0)
    charge = jnp.where(lane_row == 7, home, 0.0)
    wide = jnp.concatenate([distance, sigma, root, charge], axis=1)
    terms[...] = lax.dot_general(
        source_stack(region[pairs[2, index]]),
        home_stack(wide),
        (((0,), (0,)), ((), ())),
        preferred_element_type=jnp.float32,
    )


def strengths(terms, high, low, at_limit):
    width = terms.shape[0]
    near_at, four_at, seven_at = at_limit
    for start in range(0, width, 16):
        rows = pl.ds(start, 16)
        softened, sigma, root, charge = [
            terms[rows, k * width : (k + 1) * width] for k in range(4)
        ]
        near, four, seven = powers(jnp.minimum(softened, limit))
        square = sigma * sigma
        sixth = square * square * square
        strength = (root * sixth) * (
            sixth * (seven - seven_at) - (four - four_at)
        ) + charge * (near - near_at)
        top = strength.astype(jnp.bfloat16)
        high[rows, :] = top
        low[rows, :] = (strength - top.astype(jnp.float32)).astype(jnp.bfloat16)


def add_forces(pairs, index, region, high, low, totals):
    _, moved, _ = moved_home(pairs, index, region)
    top, middle, _ = split(region[pairs[2, index]])
    weights = stacked([top, middle])
    both = jnp.dot(weights, high[...], preferred_element_type=jnp.float32) + jnp.dot(
        weights, low[...], preferred_element_type=jnp.float32
    )
    summed = both[:ROWS] + both[ROWS:]
    totals[pairs[0, index]] += moved * summed[3:4, :] - summed


def force_kernel(pairs, count, region, out, totals, *slots):
    width = region.shape[2]
    at_limit = powers(jnp.full((16, width), limit, jnp.float32))
    totals[...] = jnp.zeros_like(totals)
    terms = (slots[:BATCH], slots[BATCH : 2 * BATCH])
    highs = (slots[2 * BATCH : 3 * BATCH], slots[3 * BATCH : 4 * BATCH])
    lows = (slots[4 * BATCH : 5 * BATCH], slots[5 * BATCH :])

    def step(index, carry):
        for turn in range(2):
            first = (2 * index + turn) * BATCH
            for t in range(BATCH):
                add_forces(pairs, first + t, region, highs[turn][t], lows[turn][t], totals)
                strengths(terms[1 - turn][t], highs[1 - turn][t], lows[1 - turn][t], at_limit)
                pair_terms(pairs, first + 2 * BATCH + t, region, terms[turn][t])
        return carry

    groups = (count[0] + BATCH - 1) // BATCH
    lax.fori_loop(0, (groups + 3) // 2, step, 0)
    for axis in range(3):
        out[axis] = totals[: out.shape[1], axis, :]


def brick_forces(region, pairs, count, blocks):
    width = region.shape[2]
    return pl.pallas_call(
        force_kernel,
        out_shape=jax.ShapeDtypeStruct((3, blocks, width), jnp.float32),
        in_specs=[
            pl.BlockSpec(memory_space=pltpu.SMEM),
            pl.BlockSpec(memory_space=pltpu.SMEM),
            pl.BlockSpec(memory_space=pltpu.VMEM),
        ],
        out_specs=pl.BlockSpec(memory_space=pltpu.VMEM),
        scratch_shapes=[pltpu.VMEM((blocks + 1, ROWS, width), jnp.float32)]
        + [pltpu.VMEM((width, 4 * width), jnp.float32)] * (2 * BATCH)
        + [pltpu.VMEM((width, width), jnp.bfloat16)] * (4 * BATCH),
    )(pairs, count, region)


def per_device(coords, charges, atom_types, lj_sigma, lj_epsilon, tile_list):
    span_y = lax.axis_size("gy")
    span_z = lax.axis_size("gz")
    blocks = coords.shape[2]
    width = coords.shape[3]
    layers = blocks // (GRID * GRID)
    ranks = span_y * span_z
    stride = blocks // ranks
    dtype = coords.dtype
    kinds = jnp.arange(lj_sigma.shape[0], dtype=jnp.int32)
    selector = (atom_types[0][:, :, None] == kinds).astype(dtype)
    sigma_atom = jnp.sum(selector * (lj_sigma * sigma_scale), axis=2)
    root_atom = jnp.sum(selector * (jnp.sqrt(lj_epsilon) * root_scale), axis=2)
    inner = coords[:, 0] - 0.5 * cell_edge
    square = inner[0] * inner[0] + inner[1] * inner[1] + inner[2] * inner[2] + soft_core
    atoms = jnp.stack(
        [inner[0], inner[1], inner[2], jnp.ones_like(square), square]
        + [sigma_atom, root_atom, charges[0] * charge_scale],
        axis=1,
    )
    outgoing = atoms.reshape(stride, ranks, ROWS, width)
    padded = exchanged(outgoing, layers)
    region = padded.reshape(-1, ROWS, width)
    pairs = jnp.pad(
        tile_list[0, 0, 0], ((0, 0), (2 * BATCH, 4 * BATCH)), constant_values=-1
    )
    dead = pairs[0] < 0

    def place(ids):
        slot = ids // blocks
        member = ids % blocks
        px = member // (GRID * layers) + (slot // 9 - 1) * GRID
        py = member // layers % GRID + (slot // 3 % 3 - 1) * GRID
        pz = member % layers + (slot % 3 - 1) * layers
        return px, py, pz

    own = place(jnp.where(dead, 0, pairs[0]) + 13 * blocks)
    other = place(jnp.where(dead, 13 * blocks, pairs[1]))
    lines = [
        ((x + 1) * (GRID + 2) + y + 1) * (layers + 2) + z + 1 for x, y, z in (own, other)
    ]
    table = jnp.stack(
        [jnp.where(dead, blocks, pairs[0])] + lines + [b - a for a, b in zip(own, other)]
    )
    count = jnp.sum((~dead).astype(jnp.int32)).reshape(1)
    totals = brick_forces(region, table, count, blocks)
    sending = totals.reshape(3, ranks, stride, width)[:, :, :, None]
    returned = lax.all_to_all(sending, ("gy", "gz"), split_axis=1, concat_axis=3, tiled=True)
    return returned.reshape(3, 1, blocks, width)


def solution(mesh):
    return jax.shard_map(
        per_device,
        mesh=mesh,
        in_specs=(
            P(None, "gx", ("gy", "gz"), None),
            P("gx", ("gy", "gz"), None),
            P("gx", ("gy", "gz"), None),
            P(),
            P(),
            P("gx", "gy", "gz", None, None),
        ),
        out_specs=P(None, "gx", ("gy", "gz"), None),
        check_vma=False,
    )
```
